32 devices in a mesh: tower: 2 (over core), tp: 4 (over z), grp: 4 (over y, x).
Axes of the slice: x: 2, y: 2, z: 4, core: 2. Of those that a mesh axis runs over, the one named last changes fastest.
Arguments:
- tokens: bfloat16 [3072, 8192], P('grp', 'tp'), may hold values from -700 to 700
- modality: int32 [3072], P('grp'), may hold values from 0 to 1, as said below
- doc_ids: int32 [3072], P('grp'), may hold values from 0 to 15, as said below
- owner_ids: int32 [3072], P('grp'), may hold values from 0 to 3, as said below
- norm_gain: float32 [2, 8192], P('tower'), may hold values from 0.5 to 1.5
- query_weight: bfloat16 [2, 8192, 4096], P('tower', 'grp', 'tp'), may hold values from -0.125 to 0.125
- pair_weight: bfloat16 [2, 8192, 1024], P('tower', 'grp'), may hold values from -0.125 to 0.125
Outputs:
- attended: bfloat16 [2, 3072, 4096], P('tower', 'grp', 'tp')
The draws below stay inside these ranges and needn't reach their ends.
Inputs may be any that keep to these rules, and one draw needn't show every extreme that they name: Every group of 768 tokens holds exactly 384 tokens of each modality. `owner_ids`: within every group each owner is named by exactly 192 tokens, and by at most 192 tokens of one modality. `doc_ids`: all tokens of one document have the same owner.
All inputs are finite; a program needn't handle non-finite values.
Results may differ from the reference program's by a relative error of at most 0.0084.
Values may be sent and summed in bfloat16 or wider, within the bound.
A program may use at most 128 MiB of HBM per device.

```python
import math
import jax
import jax.numpy as jnp
from jax import lax

D = 8192
HD = 128
HEADS = 32
KV_HEADS = 4
TOK = 768
GROUPS = 4
SLOT = 192
TOKENS = 3072


WEIGHT_EDGE = 0.125


def layout(key):
    base_key = jax.random.fold_in(key, 1234)
    perm_key, run_key, star_key, cut_key = jax.random.split(base_key, 4)
    permuted = jax.vmap(lambda subkey: jax.random.permutation(subkey, TOK))(jax.random.split(perm_key, GROUPS)).astype(jnp.int32)
    owner_table = permuted // SLOT
    position = jnp.arange(TOK, dtype=jnp.int32)
    sorted_order = jnp.argsort(owner_table * TOK + position[None, :], axis=1).astype(jnp.int32)
    placed = jnp.argsort(sorted_order, axis=1).astype(jnp.int32)
    within = placed % SLOT
    first_half = jax.random.randint(run_key, (GROUPS, GROUPS // 2), 0, SLOT + 1)
    star_owner = jax.random.randint(star_key, (), 0, GROUPS)
    forced = jnp.where(star_owner % 2 == 0, SLOT, 0)
    first_half = jnp.where(jnp.arange(GROUPS // 2)[None, :] == star_owner // 2, forced, first_half)
    image_run = jnp.stack([first_half, SLOT - first_half], axis=2).reshape(GROUPS, GROUPS)
    run_here = jnp.take_along_axis(image_run, owner_table, axis=1)
    modality_table = (within < run_here).astype(jnp.int32)
    cut_flags = (jax.random.randint(cut_key, (GROUPS, GROUPS), 0, 4) == 0).astype(jnp.int32)
    cut_flags = cut_flags.at[GROUPS - 1, :].set(1)
    cut_flags = cut_flags.at[:, 0].set(0)
    segment = jnp.cumsum(cut_flags, axis=1)
    doc_table = owner_table * GROUPS + jnp.take_along_axis(segment.T, owner_table, axis=1)
    return (modality_table.reshape(-1), doc_table.reshape(-1).astype(jnp.int32), owner_table.reshape(-1))


def column_scale(key):
    return jnp.exp(jax.random.uniform(jax.random.fold_in(key, 77), (D,), jnp.float32, 0.0, math.log(10.0)))


def draw_modality(key, part):
    return layout(key)[0]


def draw_doc_ids(key, part):
    return layout(key)[1]


def draw_owner_ids(key, part):
    return layout(key)[2]


def draw_tokens(key, part):
    row_key, noise_key = jax.random.split(jax.random.fold_in(key, 11), 2)
    columns = column_scale(key)
    row_scales = jnp.exp(jax.random.uniform(row_key, (TOKENS, 1), jnp.float32, 0.0, math.log(10.0)))
    base_draw = jax.random.normal(noise_key, (TOKENS, D), jnp.float32)
    drawn = base_draw * row_scales * columns[None, :]
    return jnp.clip(drawn, -700.0, 700.0).astype(jnp.bfloat16)


def draw_query_weight(key, part):
    drawn = jax.random.normal(jax.random.fold_in(key, 21), (2, D, HEADS * HD), jnp.float32) / math.sqrt(D)
    return jnp.clip(drawn, -WEIGHT_EDGE, WEIGHT_EDGE).astype(jnp.bfloat16)


def draw_pair_weight(key, part):
    drawn = jax.random.normal(jax.random.fold_in(key, 31), (2, D, KV_HEADS, 2, HD), jnp.float32) / math.sqrt(D)
    return jnp.clip(drawn, -WEIGHT_EDGE, WEIGHT_EDGE).reshape(2, D, KV_HEADS * 2 * HD).astype(jnp.bfloat16)


def setup_inputs(seed: int = 0) -> dict:
    seeds = jax.random.split(jax.random.key(seed), 8)
    return {
        "tokens": draw_tokens(jax.random.fold_in(seeds[7], 71), 0),
        "modality": draw_modality(jax.random.fold_in(seeds[7], 71), 0),
        "doc_ids": draw_doc_ids(jax.random.fold_in(seeds[7], 71), 0),
        "owner_ids": draw_owner_ids(jax.random.fold_in(seeds[7], 71), 0),
        "norm_gain": jnp.clip(1.0 + 0.1 * jax.random.normal(seeds[4], (2, D), jnp.float32), 0.5, 1.5),
        "query_weight": draw_query_weight(jax.random.fold_in(seeds[7], 71), 0),
        "pair_weight": draw_pair_weight(jax.random.fold_in(seeds[7], 71), 0),
    }


EPS = 1e-05
MASKED = -1e+30

def normalize(rows, gain_row):
    values = rows.astype(jnp.float32)
    inverse_rms = lax.rsqrt(lax.optimization_barrier(jnp.mean(values * values, axis=1, keepdims=True)) + EPS)
    return (values * inverse_rms * gain_row[None, :]).astype(jnp.bfloat16)

def reference(tokens, modality, doc_ids, owner_ids, norm_gain, query_weight, pair_weight):
    query_all = jnp.zeros((TOKENS, HEADS * HD), jnp.bfloat16)
    pair_all = jnp.zeros((TOKENS, KV_HEADS * 2 * HD), jnp.bfloat16)
    for tower_index in range(2):
        picked = jnp.nonzero(modality == tower_index, size=TOKENS // 2)[0].astype(jnp.int32)
        normed = normalize(tokens[picked], norm_gain[tower_index])
        query_rows = jnp.dot(normed, query_weight[tower_index], preferred_element_type=jnp.float32).astype(jnp.bfloat16)
        pair_rows = jnp.dot(normed, pair_weight[tower_index], preferred_element_type=jnp.float32).astype(jnp.bfloat16)
        query_all = query_all.at[picked].set(query_rows)
        pair_all = pair_all.at[picked].set(pair_rows)
    sharing = HEADS // KV_HEADS
    scale_factor = 1.0 / math.sqrt(HD)

    def attend(owner_index):
        members = jnp.nonzero(owner_ids == owner_index, size=TOK)[0].astype(jnp.int32)
        queries = query_all[members].astype(jnp.float32).reshape(TOK, KV_HEADS, sharing, HD)
        pair_data = pair_all[members].astype(jnp.float32).reshape(TOK, KV_HEADS, 2, HD)
        doc_rows = doc_ids[members]
        images = modality[members] == 1
        allowed = (doc_rows[:, None] == doc_rows[None, :]) & ((members[None, :] <= members[:, None]) | images[:, None] & images[None, :])
        scores = jnp.einsum('qjgd,kjd->jgqk', queries, pair_data[:, :, 0]) * scale_factor
        scores = jnp.where(allowed[None, None], scores, MASKED)
        row_max = lax.optimization_barrier(jnp.max(scores, axis=3, keepdims=True))
        powered = jnp.exp(scores - row_max)
        weights = (powered / lax.optimization_barrier(jnp.sum(powered, axis=3, keepdims=True))).astype(jnp.bfloat16)
        mixed_rows = jnp.einsum('jgqk,kjd->qjgd', weights.astype(jnp.float32), pair_data[:, :, 1])
        return (mixed_rows.astype(jnp.bfloat16).reshape(TOK, HEADS * HD), members)
    outputs, member_lists = lax.map(attend, jnp.arange(GROUPS, dtype=jnp.int32))
    attention = jnp.zeros((TOKENS, HEADS * HD), jnp.bfloat16).at[member_lists.reshape(-1)].set(outputs.reshape(TOKENS, HEADS * HD))
    towers = jnp.arange(2, dtype=jnp.int32)
    return jnp.where(modality[None, :, None] == towers[:, None, None], attention[None], jnp.zeros((), jnp.bfloat16))
```

```python
import functools
import math

import jax
import jax.numpy as jnp
from jax import lax
from jax.experimental import pallas as pl
from jax.experimental.pallas import tpu as pltpu
from jax.sharding import PartitionSpec as P

HD = 128
EPS = 1e-05
MASKED = -1e30
RUN = 16
MESH = pl.DeviceIdType.MESH
BF16, F32, I32 = jnp.bfloat16, jnp.float32, jnp.int32


def dot(a, b, contract):
    return lax.dot_general(a, b, (contract, ((), ())), preferred_element_type=F32)


def iota(shape, axis):
    return lax.broadcasted_iota(I32, shape, axis)


def joint_kernel(
    sizes,
    facts,
    tokens_hbm,
    gain_hbm,
    query_hbm,
    pair_hbm,
    ret,
    place,
    tokens,
    gain,
    weight,
    onehot,
    squares,
    squares_all,
    codes,
    codes_all,
    columns,
    chosen,
    held,
    arrived,
    normed,
    own,
    swap_out,
    swap_in,
    land,
    rows,
    kv,
    mixed,
    load_sem,
    sq_send,
    sq_recv,
    code_send,
    code_recv,
    line_send,
    line_recv,
    cross_send,
    cross_recv,
    keep_sem,
    share_send,
    share_recv,
    swap_send,
    swap_recv,
    part_send,
    part_recv,
    kv_send,
    kv_recv,
    ret_send,
    ret_recv,
    both_send,
    both_recv,
):
    groups, count, chunks, pair_heads, block = sizes
    tower, me, group = lax.axis_index("tower"), lax.axis_index("tp"), lax.axis_index("grp")
    other = 1 - tower
    tok, half = tokens.shape
    half_cols = weight.shape[2] - HD
    span = groups * RUN
    heads = half_cols // HD
    width = 2 * half
    has_left, has_right = me > 0, me < count - 1
    left, right = jnp.maximum(me - 1, 0), jnp.minimum(me + 1, count - 1)
    mine = pl.ds(pl.multiple_of(tower * half, half), half)

    barrier = pltpu.get_barrier_semaphore()
    greeted = [{"grp": lax.rem(group + k, groups)} for k in range(1, groups)]
    index = tower * count + me
    line = []
    for k in range(1, 2 * count):
        there = lax.rem(index + k, 2 * count)
        line.append((there, {"tower": there // count, "tp": lax.rem(there, count)}))
    greeted += [device for _, device in line]
    for device in greeted:
        pl.semaphore_signal(barrier, inc=1, device_id=device, device_id_type=MESH)

    token_load = pltpu.make_async_copy(tokens_hbm.at[:, mine], tokens, load_sem.at[0])
    token_load.start()
    gain_load = pltpu.make_async_copy(
        gain_hbm.at[:, pl.ds(pl.multiple_of(group * width, width), width)], gain, load_sem.at[1]
    )
    gain_load.start()
    loads = [gain_load]
    own_head = me // (count // pair_heads)
    for side in range(2):
        loads.append(
            pltpu.make_async_copy(
                query_hbm.at[:, pl.ds(side * half_cols, half_cols)],
                weight.at[side, :, pl.ds(0, half_cols)],
                load_sem.at[2 + side],
            )
        )
        loads.append(
            pltpu.make_async_copy(
                pair_hbm.at[:, pl.ds(pl.multiple_of(own_head * 2 * HD + side * HD, HD), HD)],
                weight.at[side, :, pl.ds(half_cols, HD)],
                load_sem.at[4 + side],
            )
        )
    for load in loads[1:]:
        load.start()

    owner = facts[0:1, :]
    owner_of = (iota((groups, tok), 0).astype(F32) == owner).astype(F32)
    earlier = (iota((tok, tok), 0) < iota((tok, tok), 1)).astype(F32).astype(BF16)
    ranks = dot(owner_of.astype(BF16), earlier, ((1,), (0,)))
    rank = jnp.sum(owner_of * ranks, axis=0, keepdims=True).astype(I32)
    chunk_of = lax.shift_right_logical(rank, int(math.log2(RUN)))
    spot = chunk_of * span + owner.astype(I32) * RUN + (rank - chunk_of * RUN)
    place[...] = jnp.broadcast_to(spot, place.shape)
    onehot[...] = (iota((tok, tok), 0) == spot).astype(F32).astype(BF16)

    token_load.wait()

    def choose(chunk):
        piece = onehot[pl.ds(pl.multiple_of(chunk * span, span), span), :]
        picked = dot(piece, tokens[...], ((1,), (0,))).astype(BF16)
        chosen[chunk] = picked.reshape(groups, RUN, half)

    ahead = min(3, chunks)
    for chunk in range(ahead):
        choose(chunk)

    values = tokens[...].astype(F32)
    exact = values * values
    high = exact.astype(BF16)
    low = (exact - high.astype(F32)).astype(BF16)
    ones = jnp.ones((8, half), BF16)
    squares[...] = dot(ones, high, ((1,), (1,))) + dot(ones, low, ((1,), (1,)))
    squares_all[index] = squares[...]

    pl.semaphore_wait(barrier, len(greeted))

    sq_copies = [
        pltpu.make_async_remote_copy(
            src_ref=squares,
            dst_ref=squares_all.at[index],
            send_sem=sq_send.at[k],
            recv_sem=sq_recv.at[index],
            device_id=device,
            device_id_type=MESH,
        )
        for k, (_, device) in enumerate(line)
    ]

    def hop(source, chunk, way, mine_own):
        src = chosen if mine_own else held.at[source]
        return pltpu.make_async_remote_copy(
            src_ref=src.at[chunk],
            dst_ref=held.at[source, chunk],
            send_sem=line_send.at[way, source, chunk],
            recv_sem=line_recv.at[source, chunk],
            device_id={"tp": left if way == 0 else right},
            device_id_type=MESH,
        )

    def cross(source, chunk, mine_own):
        src = chosen if mine_own else held.at[source]
        return pltpu.make_async_remote_copy(
            src_ref=src.at[chunk],
            dst_ref=arrived.at[chunk, :, group, :, mine],
            send_sem=cross_send.at[source, chunk],
            recv_sem=cross_recv.at[group, chunk],
            device_id={"grp": source},
            device_id_type=MESH,
        )

    def keep(source, chunk, mine_own):
        src = chosen if mine_own else held.at[source]
        return pltpu.make_async_copy(
            src.at[chunk], arrived.at[chunk, :, group, :, mine], keep_sem.at[chunk]
        )

    def pass_on(source, chunk, mine_own):
        @pl.when(source == group)
        def _():
            keep(source, chunk, mine_own).start()

        @pl.when(source != group)
        def _():
            cross(source, chunk, mine_own).start()

    def start_own(chunk):
        @pl.when(has_left)
        def _():
            hop(me, chunk, 0, True).start()

        @pl.when(has_right)
        def _():
            hop(me, chunk, 1, True).start()

        pass_on(me, chunk, True)

    def arrive(source, chunk, way, more):
        hop(source, chunk, way, False).wait_recv()

        @pl.when(more)
        def _():
            hop(source, chunk, way, False).start()

        pass_on(source, chunk, False)

    def arrivals(chunk, k):
        @pl.when(me + k < count)
        def _():
            arrive(me + k, chunk, 0, has_left)

        @pl.when(me - k >= 0)
        def _():
            arrive(me - k, chunk, 1, has_right)

    def share(chunk):
        return pltpu.make_async_remote_copy(
            src_ref=arrived.at[chunk, :, :, :, mine],
            dst_ref=arrived.at[chunk, :, :, :, mine],
            send_sem=share_send.at[chunk],
            recv_sem=share_recv.at[chunk],
            device_id={"tower": other},
            device_id_type=MESH,
        )

    def gathered(chunk):
        for k in range(1, groups):
            source = lax.rem(group + k, groups)
            pltpu.make_async_copy(
                chosen.at[chunk], arrived.at[chunk, :, source, :, mine], cross_recv.at[source, chunk]
            ).wait()
        keep(group, chunk, False).wait()
        share(chunk).start()

    def swap(chunk):
        return pltpu.make_async_remote_copy(
            src_ref=swap_out.at[chunk],
            dst_ref=swap_in.at[chunk],
            send_sem=swap_send.at[chunk],
            recv_sem=swap_recv.at[chunk],
            device_id={"tower": other},
            device_id_type=MESH,
        )

    def project(chunk):
        share(chunk).wait_recv()

        @pl.loop(0, groups)
        def _(o):
            scale = columns[chunk, o].reshape(span, 8)[:, 0:1]
            x = arrived[chunk, o].reshape(span, width).astype(F32)
            normed[pl.ds(pl.multiple_of(o * span, span), span), :] = (x * scale * gain[...]).astype(BF16)

        sent = dot(normed[...], weight[other], ((1,), (0,)))
        swap_out[chunk] = sent.astype(BF16).reshape(groups, span, half_cols + HD)
        kept = dot(normed[...], weight[tower], ((1,), (0,)))
        own[...] = kept.reshape(groups, span, half_cols + HD)
        swap(chunk).start()

    def part(o, chunk):
        return pltpu.make_async_remote_copy(
            src_ref=swap_out.at[chunk, o],
            dst_ref=land.at[group, chunk],
            send_sem=part_send.at[o, chunk],
            recv_sem=part_recv.at[group, chunk],
            device_id={"grp": o},
            device_id_type=MESH,
        )

    def combine(chunk):
        swap(chunk).wait()

        @pl.loop(0, groups)
        def _(o):
            kind = columns[chunk, o].reshape(span, 8)[:, 1:2]
            got = swap_in[chunk, o].astype(F32)
            swap_out[chunk, o] = jnp.where(kind == tower.astype(F32), own[o], got).astype(BF16)

        for k in range(1, groups):
            part(lax.rem(group + k, groups), chunk).start()
        land[group, chunk] = swap_out[chunk, group]

    def give_kv(chunk):
        return pltpu.make_async_remote_copy(
            src_ref=kv.at[tower, chunk],
            dst_ref=kv.at[tower, chunk],
            send_sem=kv_send.at[chunk],
            recv_sem=kv_recv.at[chunk],
            device_id={"tower": other},
            device_id_type=MESH,
        )

    def total(chunk):
        for k in range(1, groups):
            source = lax.rem(group + k, groups)
            pltpu.make_async_copy(
                swap_out.at[chunk, source], land.at[source, chunk], part_recv.at[source, chunk]
            ).wait()
        summed = land[0, chunk].astype(F32)
        for source in range(1, groups):
            summed += land[source, chunk].astype(F32)
        summed = summed.astype(BF16)
        rows[chunk] = summed[:, :half_cols]
        kv[tower, chunk] = summed[:, half_cols:]
        give_kv(chunk).start()

    for chunk in range(min(ahead, 2)):
        start_own(chunk)
    for copy in sq_copies:
        copy.start()

    for there, _ in line:
        pltpu.make_async_copy(squares, squares_all.at[there], sq_recv.at[there]).wait()
    sum_squares = squares_all[0][0:1, :]
    for k in range(1, 2 * count):
        sum_squares += squares_all[k][0:1, :]
    inverse = lax.rsqrt(sum_squares / (width * count) + EPS)
    inverse_high = inverse.astype(BF16).astype(F32)
    rest = inverse - inverse_high
    inverse_mid = rest.astype(BF16).astype(F32)
    inverse_low = rest - inverse_mid
    position = iota((1, tok), 1)
    position_high = lax.shift_right_logical(position, 5)
    position_low = position - position_high * 32
    row = iota((16, tok), 0)
    stack = jnp.zeros((16, tok), F32)
    for k, line_values in enumerate(
        (
            inverse_high,
            inverse_mid,
            inverse_low,
            facts[1:2, :],
            facts[2:3, :],
            position_high.astype(F32),
            position_low.astype(F32),
        )
    ):
        stack = jnp.where(row == k, line_values, stack)
    ordered = dot(stack.astype(BF16), onehot[...], ((1,), (1,)))
    row = iota((8, tok), 0)
    packed = jnp.where(row == 0, ordered[0:1] + ordered[1:2] + ordered[2:3], 0.0)
    packed = jnp.where(row == 1, ordered[3:4], packed)
    packed = jnp.where(row == 2, ordered[4:5], packed)
    global_position = ordered[5:6] * 32.0 + ordered[6:7] + (group * tok).astype(F32)
    packed = jnp.where(row == 3, global_position, packed)
    codes[...] = packed
    codes_all[group] = packed

    def code_copy(k):
        return pltpu.make_async_remote_copy(
            src_ref=codes,
            dst_ref=codes_all.at[group],
            send_sem=code_send.at[k - 1],
            recv_sem=code_recv.at[group],
            device_id={"grp": lax.rem(group + k, groups)},
            device_id_type=MESH,
        )

    for k in range(1, groups):
        code_copy(k).start()

    def finish_codes():
        for load in loads:
            load.wait()
        for k in range(1, groups):
            source = lax.rem(group + k, groups)
            pltpu.make_async_copy(codes, codes_all.at[source], code_recv.at[source]).wait()
        for g in range(groups):
            columns[:, :, g] = jnp.transpose(codes_all[g]).reshape(chunks, groups, RUN, 8)

    def step(chunk):
        @pl.when(chunk + 2 < chunks)
        def _():
            start_own(chunk + 2)

        @pl.when(chunk + ahead < chunks)
        def _():
            choose(chunk + ahead)

        def stage_gather():
            @pl.when((chunk >= 1) & (chunk <= chunks))
            def _():
                gathered(chunk - 1)

        def stage_project():
            @pl.when((chunk >= 1) & (chunk <= chunks))
            def _():
                project(chunk - 1)

        for k in range(1, count):

            @pl.when(chunk < chunks)
            def _():
                arrivals(chunk, k)

            if k == 1:
                stage_gather()
            if k == min(2, count - 1):
                stage_project()

        @pl.when(chunk == 0)
        def _():
            finish_codes()

        @pl.when((chunk >= 1) & (chunk <= chunks))
        def _():
            combine(chunk - 1)

        @pl.when(chunk >= 2)
        def _():
            total(chunk - 2)

    @pl.loop(0, chunks + 2)
    def _(chunk):
        step(chunk)

    @pl.loop(0, chunks)
    def _(chunk):
        give_kv(chunk).wait_recv()

    total_rows = chunks * span
    facts_row = jnp.transpose(columns[:, group].reshape(total_rows, 8))
    kind_k, doc_k, place_k = facts_row[1:2], facts_row[2:3], facts_row[3:4]

    def back(target, part_block, to_grp):
        chunk = pl.ds(part_block * block, block)
        return pltpu.make_async_remote_copy(
            src_ref=mixed.at[chunk, target],
            dst_ref=ret.at[chunk, group, :, pl.ds(pl.multiple_of(tower * half_cols, half_cols), half_cols)],
            send_sem=ret_send.at[target, part_block],
            recv_sem=ret_recv.at[group, part_block],
            device_id={"grp": to_grp},
            device_id_type=MESH,
        )

    def back_local(part_block):
        chunk = pl.ds(part_block * block, block)
        return pltpu.make_async_copy(
            mixed.at[chunk, group],
            ret.at[chunk, group, :, pl.ds(pl.multiple_of(tower * half_cols, half_cols), half_cols)],
            ret_recv.at[group, part_block],
        )

    def both(source, part_block):
        chunk = pl.ds(part_block * block, block)
        where = ret.at[chunk, source, :, pl.ds(pl.multiple_of(tower * half_cols, half_cols), half_cols)]
        return pltpu.make_async_remote_copy(
            src_ref=where,
            dst_ref=where,
            send_sem=both_send.at[source, part_block],
            recv_sem=both_recv.at[source, part_block],
            device_id={"tower": other},
            device_id_type=MESH,
        )

    keys = kv.at[0]
    vals = kv.at[1]

    def attend(chunk):
        query = jnp.concatenate([rows[chunk, :, h * HD : (h + 1) * HD] for h in range(heads)], axis=0)
        column = columns[chunk, group].reshape(span, 8)
        kind_q, doc_q, place_q = column[:, 1:2], column[:, 2:3], column[:, 3:4]
        same = doc_q == doc_k
        seen = (place_k <= place_q) | ((kind_q + kind_k) == 2.0)
        bias = jnp.where(same & seen, 0.0, MASKED)
        scores = dot(query, keys[...].reshape(total_rows, HD), ((1,), (1,)))
        scores = scores * (1.0 / math.sqrt(HD)) + jnp.concatenate([bias] * heads, axis=0)
        powered = jnp.exp(scores - jnp.max(scores, axis=1, keepdims=True))
        weights = (powered / jnp.sum(powered, axis=1, keepdims=True)).astype(BF16)
        out = dot(weights, vals[...].reshape(total_rows, HD), ((1,), (0,))).astype(BF16)
        for h in range(heads):
            mixed[chunk, :, :, h * HD : (h + 1) * HD] = out[h * span : (h + 1) * span].reshape(groups, RUN, HD)

    blocks = chunks // block

    @pl.loop(0, blocks)
    def _(part_block):
        @pl.loop(0, block)
        def _(inner):
            attend(part_block * block + inner)

        for k in range(1, groups):
            target = lax.rem(group + k, groups)
            back(target, part_block, target).start()
        back_local(part_block).start()

    @pl.loop(0, blocks)
    def _(part_block):
        for k in range(1, groups):
            source = lax.rem(group + k, groups)
            pltpu.make_async_copy(
                mixed.at[pl.ds(part_block * block, block), source],
                ret.at[
                    pl.ds(part_block * block, block),
                    source,
                    :,
                    pl.ds(pl.multiple_of(tower * half_cols, half_cols), half_cols),
                ],
                ret_recv.at[source, part_block],
            ).wait()
            both(source, part_block).start()
        back_local(part_block).wait()
        both(group, part_block).start()

    for copy in sq_copies:
        copy.wait_send()
    for k in range(1, groups):
        code_copy(k).wait_send()

    @pl.loop(0, chunks)
    def _(chunk):
        for source in range(count):

            @pl.when(source != group)
            def _():
                cross(source, chunk, False).wait_send()

            @pl.when((source >= me) & has_left)
            def _():
                hop(source, chunk, 0, False).wait_send()

            @pl.when((source <= me) & has_right)
            def _():
                hop(source, chunk, 1, False).wait_send()

        share(chunk).wait_send()
        give_kv(chunk).wait_send()
        for k in range(1, groups):
            part(lax.rem(group + k, groups), chunk).wait_send()

    @pl.loop(0, blocks)
    def _(part_block):
        for k in range(1, groups):
            target = lax.rem(group + k, groups)
            back(target, part_block, target).wait_send()
        for source in range(groups):
            both(source, part_block).wait_recv()
            both(source, part_block).wait_send()


def joint(facts, tokens, gain, query_weight, pair_weight, groups, count, heads_total):
    tok, width = tokens.shape
    half = width // 2
    head_cols = query_weight.shape[1]
    half_cols = head_cols // 2
    cols = half_cols + HD
    slots = tok // groups
    chunks = slots // RUN
    span = groups * RUN
    block = chunks // 4 if chunks % 4 == 0 else 1
    blocks = chunks // block
    vmem = pl.BlockSpec(memory_space=pltpu.VMEM)
    hbm = pl.BlockSpec(memory_space=pl.ANY)
    dma = pltpu.SemaphoreType.DMA
    return pl.pallas_call(
        functools.partial(joint_kernel, (groups, count, chunks, heads_total, block)),
        out_shape=[
            jax.ShapeDtypeStruct((chunks, groups, RUN, head_cols), BF16),
            jax.ShapeDtypeStruct((8, tok), I32),
        ],
        in_specs=[vmem, hbm, hbm, hbm, hbm],
        out_specs=[vmem, vmem],
        scratch_shapes=[
            pltpu.VMEM((tok, half), BF16),
            pltpu.VMEM((1, width), F32),
            pltpu.VMEM((2, width, cols), BF16),
            pltpu.VMEM((tok, tok), BF16),
            pltpu.VMEM((8, tok), F32),
            pltpu.VMEM((2 * count, 8, tok), F32),
            pltpu.VMEM((8, tok), F32),
            pltpu.VMEM((groups, 8, tok), F32),
            pltpu.VMEM((chunks, groups, groups, RUN, 8), F32),
            pltpu.VMEM((chunks, groups, RUN, half), BF16),
            pltpu.VMEM((count, chunks, groups, RUN, half), BF16),
            pltpu.VMEM((chunks, groups, groups, RUN, width), BF16),
            pltpu.VMEM((groups * span, width), BF16),
            pltpu.VMEM((groups, span, cols), F32),
            pltpu.VMEM((chunks, groups, span, cols), BF16),
            pltpu.VMEM((chunks, groups, span, cols), BF16),
            pltpu.VMEM((groups, chunks, span, cols), BF16),
            pltpu.VMEM((chunks, span, half_cols), BF16),
            pltpu.VMEM((2, chunks, span, HD), BF16),
            pltpu.VMEM((chunks, groups, RUN, half_cols), BF16),
            dma((6,)),
            dma((2 * count,)),
            dma((2 * count,)),
            dma((groups,)),
            dma((groups,)),
            dma((2, count, chunks)),
            dma((count, chunks)),
            dma((count, chunks)),
            dma((groups, chunks)),
            dma((chunks,)),
            dma((chunks,)),
            dma((chunks,)),
            dma((chunks,)),
            dma((chunks,)),
            dma((groups, chunks)),
            dma((groups, chunks)),
            dma((chunks,)),
            dma((chunks,)),
            dma((groups, blocks)),
            dma((groups, blocks)),
            dma((groups, blocks)),
            dma((groups, blocks)),
        ],
        compiler_params=pltpu.CompilerParams(
            collective_id=1, has_side_effects=True, vmem_limit_bytes=63 * 2**20
        ),
        name="joint",
    )(facts, tokens, gain, query_weight, pair_weight)


def local(tokens, modality, doc_ids, owner_ids, norm_gain, query_weight, pair_weight):
    groups = lax.axis_size("grp")
    count = lax.axis_size("tp")
    tower = lax.axis_index("tower")
    tok = tokens.shape[0]
    head_cols = query_weight.shape[2]
    pair_heads = pair_weight.shape[2] // (2 * HD)
    row = jnp.arange(8, dtype=I32)[:, None]
    facts = jnp.where(
        row == 0, owner_ids[None], jnp.where(row == 1, modality[None], jnp.where(row == 2, doc_ids[None], 0))
    ).astype(F32)
    ret, place = joint(
        facts, tokens, norm_gain, query_weight[0], pair_weight[0], groups, count, pair_heads
    )
    ret = ret.reshape(tok, head_cols)
    chosen = (place[0][:, None] == jnp.arange(tok, dtype=I32)[None, :]) & (modality == tower)[:, None]
    result = jnp.dot(chosen.astype(BF16), ret, preferred_element_type=F32).astype(BF16)
    return result[None]


def solution(mesh):
    in_specs = (
        P("grp", "tp"),
        P("grp"),
        P("grp"),
        P("grp"),
        P("tower", None),
        P("tower", "grp", "tp"),
        P("tower", "grp", None),
    )
    out_specs = P("tower", "grp", "tp")
    return jax.shard_map(local, mesh=mesh, in_specs=in_specs, out_specs=out_specs, check_vma=False)
```
